32 devices in a mesh: dp: 2 (over x), expert: 16 (over z, y, core).
Axes of the slice: x: 2, y: 2, z: 4, core: 2. Of those that a mesh axis runs over, the one named last changes fastest.
Arguments:
- gradients: bfloat16 [16, 1024, 5888], P(None, ('dp', 'expert')), may hold values from -6 to 6
- momentum: bfloat16 [16, 1024, 5888], P('expert', 'dp'), may hold values from -6 to 6
- right_factor: bfloat16 [16, 5888, 256], P('expert', 'dp'), may hold values from -6 to 6
Outputs:
- new_momentum: bfloat16 [16, 1024, 5888], P('expert', 'dp')
- new_factor: bfloat16 [16, 5888, 256], P('expert', 'dp')
- update_rows: bfloat16 [16, 1024, 5888], P(None, ('dp', 'expert'))
The draws below stay inside these ranges and needn't reach their ends.
All inputs are finite; a program needn't handle non-finite values.
Results may differ from the reference program's by a relative error of at most 0.009.
Values may be sent and summed in bfloat16 or wider, within the bound.
A program may use at most 128 MiB of HBM per device.

```python
import math
import jax
import jax.numpy as jnp
from jax import lax

D = 5888
FFW = 1024
RANK = 256
EXPERTS = 16


def levels(own_key, dims, pieces, smallest, top_value):
    gain = 1.0
    for dim, blocks in pieces:
        heights = jax.random.uniform(jax.random.fold_in(jax.random.fold_in(own_key, 6), dim), (blocks,), jnp.float32, smallest / len(pieces), top_value / len(pieces))
        gain = gain * jnp.repeat(jnp.exp(heights), dims[dim] // blocks).reshape((-1,) + (1,) * (len(dims) - 1 - dim))
    return gain


def scatter_about(own_key, dims, width, limit, pieces=(), kind=jnp.bfloat16):
    array = width * jax.random.normal(own_key, dims, jnp.float32)
    if pieces:
        array = array * levels(own_key, dims, pieces, -0.22, 0.18)
    return jnp.clip(array, -limit, limit).astype(kind)


def setup_inputs(seed: int = 0) -> dict:
    arg_keys = jax.random.split(jax.random.key(seed), 4)
    return {
        "gradients": scatter_about(arg_keys[0], (EXPERTS, FFW, D), 1.0, 6.0, ((1, 32),)),
        "momentum": scatter_about(arg_keys[1], (EXPERTS, FFW, D), 1.0, 6.0, ((0, 16), (1, 2))),
        "right_factor": scatter_about(arg_keys[2], (EXPERTS, D, RANK), 1.0, 6.0, ((0, 16), (1, 2))),
    }


decay_rate = 0.95
epsilon = 1e-06

def one_expert(items):
    grad_rows, moment_rows, factor = items
    blended = (decay_rate * moment_rows.astype(jnp.float32) + grad_rows.astype(jnp.float32)).astype(jnp.bfloat16)
    left = jnp.dot(blended.astype(jnp.float32), factor.astype(jnp.float32), preferred_element_type=jnp.float32)
    gram_matrix = jnp.dot(left.T, left, precision=lax.Precision.HIGHEST)
    lower = jnp.linalg.cholesky(gram_matrix)
    inverse = jax.scipy.linalg.solve_triangular(lower, jnp.eye(RANK, dtype=jnp.float32), lower=True)
    ortho = jnp.dot(left, inverse.T, precision=lax.Precision.HIGHEST).astype(jnp.bfloat16)
    right = lax.dot_general(blended.astype(jnp.float32), ortho.astype(jnp.float32), (((0,), (0,)), ((), ())), preferred_element_type=jnp.float32)
    right_rounded = right.astype(jnp.bfloat16)
    kept = (blended.astype(jnp.float32) - (1.0 - decay_rate) * lax.dot_general(ortho.astype(jnp.float32), right_rounded.astype(jnp.float32), (((1,), (1,)), ((), ())), preferred_element_type=jnp.float32)).astype(jnp.bfloat16)
    column = lax.optimization_barrier(jnp.sum(right * right, axis=0))
    new_factor = (right * lax.rsqrt(column / D + epsilon)).astype(jnp.bfloat16)
    update = (math.sqrt(FFW / RANK) * lax.dot_general(ortho.astype(jnp.float32), new_factor.astype(jnp.float32), (((1,), (1,)), ((), ())), preferred_element_type=jnp.float32)).astype(jnp.bfloat16)
    return (kept, new_factor, update)

def reference(gradients, momentum, right_factor):
    kept, new_factor, update = lax.map(one_expert, (gradients, momentum, right_factor))
    return (kept, new_factor, update)
```

```python
import functools
import math

import jax
import jax.numpy as jnp
from jax import lax
from jax.experimental import pallas as pl
from jax.experimental.pallas import tpu as pltpu
from jax.sharding import PartitionSpec as P

decay_rate = 0.95
epsilon = 1e-06
PIECES = 4
LANES = 128
SIDE = 8
MESH = pl.DeviceIdType.MESH


def exact_dot(a, b, contract):
    return lax.dot_general(
        a,
        b,
        (((contract[0],), (contract[1],)), ((), ())),
        precision=lax.Precision.HIGHEST,
        preferred_element_type=jnp.float32,
    )


def dot(a, b, contract=(1, 0)):
    return lax.dot_general(
        a, b, (((contract[0],), (contract[1],)), ((), ())), preferred_element_type=jnp.float32
    )


def factor_inverse(work, rank):
    block = min(LANES, rank)
    wide = 2 * rank // LANES
    sub = lax.broadcasted_iota(jnp.int32, (SIDE, LANES), 0)
    lane = lax.broadcasted_iota(jnp.int32, (SIDE, block), 1)
    place = lax.broadcasted_iota(jnp.int32, (block, 2 * rank), 0)
    for start in range(0, rank, block):

        def panel(step, _, start=start):
            first = pl.multiple_of(step * SIDE, SIDE)
            rows = work[pl.ds(start + first, SIDE), :]
            square = rows[:, start : start + block]
            columns = [
                jnp.broadcast_to(
                    jnp.sum(jnp.where(lane == first + j, square, 0.0), axis=1, keepdims=True),
                    (SIDE, LANES),
                )
                for j in range(SIDE)
            ]
            subs = jnp.concatenate([sub] * wide, axis=1)
            for j in range(SIDE):
                root = lax.rsqrt(jnp.broadcast_to(columns[j][j : j + 1, :], (SIDE, LANES)))
                column = columns[j] * root
                pivot = jnp.broadcast_to(rows[j : j + 1, :], rows.shape)
                pivot = pivot * jnp.concatenate([root] * wide, axis=1)
                below = rows - jnp.concatenate([column] * wide, axis=1) * pivot
                rows = jnp.where(subs == j, pivot, jnp.where(subs > j, below, rows))
                for k in range(j + 1, SIDE):
                    columns[k] = columns[k] - column * jnp.broadcast_to(
                        column[k : k + 1, :], (SIDE, LANES)
                    )
            work[pl.ds(start + first, SIDE), :] = rows
            change = exact_dot(rows[:, start : start + block], rows, (0, 0))
            old = work[start : start + block, :]
            work[start : start + block, :] = jnp.where(place >= first + SIDE, old - change, old)
            return 0

        lax.fori_loop(0, block // SIDE, panel, 0)
        if start + block < rank:
            done = work[start : start + block, :]
            work[start + block :, :] = work[start + block :, :] - exact_dot(
                done[:, start + block : rank], done, (0, 0)
            )


def cuts(depth):
    tiles = depth // LANES
    pieces = min(PIECES, tiles)
    edges = [-(-tiles * k // pieces) * LANES for k in range(pieces + 1)]
    return list(zip(edges[:-1], edges[1:]))


def step_kernel(
    dp,
    experts,
    layers,
    gradients,
    momentum,
    right_factor,
    kept_out,
    factor_out,
    update_out,
    blended,
    held,
    factor,
    other,
    left,
    work,
    ortho,
    right,
    rounded,
    normal,
    rows_in,
    update,
    turned,
    sums,
    grad_send,
    grad_recv,
    half_send,
    half_recv,
    left_send,
    left_recv,
    pair_send,
    pair_recv,
    sum_send,
    sum_recv,
    round_send,
    round_recv,
    rows_send,
    rows_recv,
    normal_send,
    normal_recv,
    update_send,
    update_recv,
    local_sem,
):
    x = lax.axis_index("dp")
    e = lax.axis_index("expert")
    group = experts // layers
    z, s = e // group, lax.rem(e, group)
    few = gradients.shape[1]
    rows, width = momentum.shape
    depth, rank = right_factor.shape
    team = dp * group
    mine = x * group + s
    pieces = cuts(depth)

    def remote(src, dst, send, recv, to_x, to_e):
        return pltpu.make_async_remote_copy(
            src_ref=src,
            dst_ref=dst,
            send_sem=send,
            recv_sem=recv,
            device_id=(to_x, to_e),
            device_id_type=MESH,
        )

    def mate(k):
        return lax.rem(x + k, dp)

    def away(t):
        apart = (t + 1) // 2
        to = jnp.where(lax.rem(t, 2) == 1, z + apart, z - apart)
        return to, (to >= 0) & (to < layers)

    barrier = pltpu.get_barrier_semaphore()

    def greet_expert(k, _):
        pl.semaphore_signal(
            barrier, inc=1, device_id=(x, lax.rem(e + k, experts)), device_id_type=MESH
        )
        return 0

    lax.fori_loop(1, experts, greet_expert, 0)
    for k in range(1, dp):
        for m in range(group):
            pl.semaphore_signal(
                barrier, inc=1, device_id=(mate(k), z * group + m), device_id_type=MESH
            )
    local_momentum = pltpu.make_async_copy(momentum, held, local_sem.at[0])
    local_momentum.start()
    local_factor = pltpu.make_async_copy(right_factor, factor.at[x], local_sem.at[1])
    local_factor.start()
    local_grad = pltpu.make_async_copy(gradients.at[e], blended.at[e], local_sem.at[2])
    local_grad.start()
    pl.semaphore_wait(barrier, experts - 1 + (dp - 1) * group)

    factor_copies = [
        remote(right_factor, factor.at[x], pair_send.at[k - 1], pair_recv.at[k - 1], mate(k), e)
        for k in range(1, dp)
    ]
    for copy in factor_copies:
        copy.start()

    def grad_copy(to):
        return remote(
            gradients.at[to], blended.at[e], grad_send.at[to], grad_recv.at[e], x, to
        )

    def send_layer(t, _):
        to, real = away(2 * (layers - 1) - t)

        @pl.when(real)
        def _():
            def one(k, _):
                m = lax.rem(s + k, group)

                @pl.when(to * group + m != e)
                def _():
                    grad_copy(to * group + m).start()

                return 0

            lax.fori_loop(0, group, one, 0)

        return 0

    lax.fori_loop(0, 2 * layers - 1, send_layer, 0)
    local_momentum.wait()
    local_factor.wait()
    local_grad.wait()
    for copy in factor_copies:
        copy.wait_recv()

    def half_copy(k, block):
        to = mate(k)
        return remote(
            blended.at[block, :, pl.ds(pl.multiple_of(to * depth, LANES), depth)],
            other.at[k - 1, block],
            half_send.at[k - 1, block],
            half_recv.at[k - 1, block],
            to,
            e,
        )

    def left_copy(k, block):
        part = left.at[x, pl.ds(pl.multiple_of(block * few, few), few)]
        return remote(
            part, part, left_send.at[k - 1, block], left_recv.at[k - 1, block], mate(k), e
        )

    def take_layer(t, _):
        source, real = away(t)

        @pl.when(real)
        def _():
            def one(k, _):
                block = source * group + lax.rem(s + group - k, group)

                @pl.when(block != e)
                def _():
                    remote(
                        gradients.at[block], blended.at[block],
                        grad_send.at[block], grad_recv.at[block], x, block,
                    ).wait_recv()

                span = pl.ds(pl.multiple_of(block * few, few), few)
                new = (
                    decay_rate * held[span].astype(jnp.float32)
                    + blended[block].astype(jnp.float32)
                ).astype(jnp.bfloat16)
                blended[block] = new
                left[x, span] = dot(new, factor[...].reshape(dp * depth, rank))
                for k in range(1, dp):
                    half_copy(k, block).start()
                    left_copy(k, block).start()
                return 0

            lax.fori_loop(0, group, one, 0)

        return 0

    lax.fori_loop(0, 2 * layers - 1, take_layer, 0)

    def arrived(block, _):
        for k in range(1, dp):
            half_copy(k, block).wait_recv()
            left_copy(k, block).wait_recv()
        return 0

    lax.fori_loop(0, experts, arrived, 0)

    every = left[...].reshape(dp * rows, rank)
    row = lax.broadcasted_iota(jnp.int32, (rank, rank), 0)
    col = lax.broadcasted_iota(jnp.int32, (rank, rank), 1)
    work[:, :rank] = exact_dot(every, every, (0, 0))
    work[:, rank:] = jnp.where(row == col, 1.0, 0.0)
    factor_inverse(work, rank)
    inverse = work[:, rank:]
    for k in range(dp):
        ortho[k] = exact_dot(left[k], inverse, (1, 1)).astype(jnp.bfloat16)
    per = group * few

    def rows_copy(source, to):
        return remote(
            ortho.at[:, pl.ds(pl.multiple_of(to * per, per), per)],
            rows_in.at[source],
            rows_send.at[to],
            rows_recv.at[source],
            x,
            to * group + s,
        )

    def send_rows(t, _):
        to, real = away(t)

        @pl.when(real)
        def _():
            rows_copy(z, to).start()

        return 0

    own = jnp.transpose(exact_dot(left[x], inverse, (1, 1))).astype(jnp.bfloat16)
    others = [
        jnp.transpose(exact_dot(left[mate(k)], inverse, (1, 1))).astype(jnp.bfloat16)
        for k in range(1, dp)
    ]
    square = jnp.zeros((SIDE, rank), jnp.float32)
    for lo, hi in pieces:
        begin = pl.multiple_of(x * depth + lo, LANES)
        part = dot(own, blended[:, :, pl.ds(begin, hi - lo)].reshape(rows, hi - lo))
        for k in range(1, dp):
            part = part + dot(others[k - 1], other[k - 1, :, :, lo:hi].reshape(rows, hi - lo))
        right[:, lo:hi] = part
        rounded[x, :, lo:hi] = part.astype(jnp.bfloat16)
        square = square + exact_dot(
            jnp.ones((SIDE, hi - lo), jnp.float32), part * part, (1, 1)
        )
    sums[0] = square
    lax.fori_loop(1, 2 * layers - 1, send_rows, 0)
    sum_copies = [
        remote(sums.at[0], sums.at[k], sum_send.at[k - 1], sum_recv.at[k - 1], mate(k), e)
        for k in range(1, dp)
    ]
    for copy in sum_copies:
        copy.start()
    round_copies = [
        remote(rounded.at[x], rounded.at[x], round_send.at[k - 1], round_recv.at[k - 1], mate(k), e)
        for k in range(1, dp)
    ]
    for copy in round_copies:
        copy.start()
    total = square
    for k in range(1, dp):
        sum_copies[k - 1].wait_recv()
        total = total + sums[k]
    scale = lax.rsqrt(total[0:1, :] / width + epsilon)
    scale = jnp.transpose(jnp.broadcast_to(scale, (LANES, rank)))[:, 0:1]

    def normal_copy(layer, piece, side):
        lo, hi = pieces[piece]
        part = normal.at[layer, :, lo:hi]
        to = jnp.clip(z + side, 0, layers - 1)
        return remote(
            part,
            part,
            normal_send.at[layer, piece, (side + 1) // 2],
            normal_recv.at[layer, piece],
            x,
            to * group + s,
        )

    def update_copy(layer, piece, k):
        lo, hi = pieces[piece]
        to = lax.rem(mine + k, team)
        to_x, to_s = to // group, lax.rem(to, group)
        return (
            update.at[layer, to_x, pl.ds(pl.multiple_of(to_s * few, few), few), lo:hi],
            update_out.at[
                layer * group + s, :, pl.ds(pl.multiple_of(x * depth + lo, LANES), hi - lo)
            ],
            to_x,
            z * group + to_s,
        )

    def multiply(layer, piece):
        lo, hi = pieces[piece]
        result = math.sqrt(rows * dp / rank) * dot(
            rows_in[layer].reshape(dp * per, rank), normal[layer, :, lo:hi]
        )
        update[layer, :, :, lo:hi] = result.astype(jnp.bfloat16).reshape(dp, per, hi - lo)

    def scatter(layer, piece):
        src, dst, _, _ = update_copy(layer, piece, 0)
        pltpu.make_async_copy(src, dst, update_recv.at[layer, mine]).start()

        def one(k, _):
            src, dst, to_x, to_e = update_copy(layer, piece, k)
            remote(
                src, dst, update_send.at[layer, k - 1], update_recv.at[layer, mine], to_x, to_e
            ).start()
            return 0

        lax.fori_loop(1, team, one, 0)

    for piece, (lo, hi) in enumerate(pieces):
        normal[z, :, lo:hi] = (right[:, lo:hi] * scale).astype(jnp.bfloat16)
    rows_in[z] = ortho[:, pl.ds(pl.multiple_of(z * per, per), per)]
    for piece in range(len(pieces)):
        multiply(z, piece)
        for side in (1, -1):

            @pl.when((z + side >= 0) & (z + side < layers))
            def _(piece=piece, side=side):
                normal_copy(z, piece, side).start()

    for piece in range(len(pieces)):
        scatter(z, piece)

    turned[...] = jnp.transpose(normal[z].astype(jnp.float32)).astype(jnp.bfloat16)
    factor_store = pltpu.make_async_copy(turned, factor_out, local_sem.at[1])
    factor_store.start()
    for copy in round_copies:
        copy.wait_recv()
    own_rows = ortho[x]
    for k in range(dp):
        for lo, hi in pieces:
            at = slice(k * depth + lo, k * depth + hi)
            old = blended[:, :, at].reshape(rows, hi - lo).astype(jnp.float32)
            held[:, at] = (
                old - (1.0 - decay_rate) * dot(own_rows, rounded[k, :, lo:hi])
            ).astype(jnp.bfloat16)
    kept_store = pltpu.make_async_copy(held, kept_out, local_sem.at[0])
    kept_store.start()

    def far(apart, _):
        for side in (1, -1):
            layer = z - side * apart

            @pl.when((layer >= 0) & (layer < layers))
            def _():
                rows_copy(layer, z).wait_recv()

        for piece in range(len(pieces)):
            for side in (1, -1):
                layer = z - side * apart

                @pl.when((layer >= 0) & (layer < layers))
                def _(piece=piece, side=side, layer=layer):
                    normal_copy(layer, piece, side).wait_recv()

                    @pl.when((z + side >= 0) & (z + side < layers))
                    def _():
                        normal_copy(layer, piece, side).start()

                    multiply(layer, piece)
                    scatter(layer, piece)

        return 0

    lax.fori_loop(1, layers, far, 0)

    def done_block(block, _):
        @pl.when(block != e)
        def _():
            grad_copy(block).wait_send()

        for k in range(1, dp):
            half_copy(k, block).wait_send()
            left_copy(k, block).wait_send()
        return 0

    lax.fori_loop(0, experts, done_block, 0)
    for copy in factor_copies + sum_copies + round_copies:
        copy.wait_send()

    def done_layer(layer, _):
        @pl.when(layer != z)
        def _():
            rows_copy(z, layer).wait_send()

        for piece in range(len(pieces)):
            for side in (1, -1):

                @pl.when((side * (z - layer) >= 0) & (z + side >= 0) & (z + side < layers))
                def _(piece=piece, side=side):
                    normal_copy(layer, piece, side).wait_send()

        def one(k, _):
            src = update.at[layer, 0, pl.ds(0, few)]
            dst = update_out.at[layer * group, :, pl.ds(0, depth)]
            remote(
                src, dst, update_send.at[layer, k - 1], update_recv.at[layer, mine], mate(1), e
            ).wait_send()
            return 0

        lax.fori_loop(1, team, one, 0)

        def come(m, _):
            src = update.at[layer, 0, pl.ds(0, few)]
            dst = update_out.at[layer * group, :, pl.ds(0, depth)]
            pltpu.make_async_copy(src, dst, update_recv.at[layer, m]).wait()
            return 0

        lax.fori_loop(0, team, come, 0)
        return 0

    lax.fori_loop(0, layers, done_layer, 0)
    factor_store.wait()
    kept_store.wait()


def make_body(dp):
    def body(gradients, momentum, right_factor):
        experts, few, width = gradients.shape
        rows = momentum.shape[1]
        depth, rank = right_factor.shape[1:]
        group = max(1, min(experts, rank // (dp * few)))
        while experts % group:
            group -= 1
        layers = experts // group
        team = dp * group
        pieces = len(cuts(depth))
        any_space = pl.BlockSpec(memory_space=pl.ANY)
        bf16, f32 = jnp.bfloat16, jnp.float32
        dma = pltpu.SemaphoreType.DMA
        kept, own_factor, returned = pl.pallas_call(
            functools.partial(step_kernel, dp, experts, layers),
            out_shape=(
                jax.ShapeDtypeStruct((rows, width), bf16),
                jax.ShapeDtypeStruct((depth, rank), bf16),
                jax.ShapeDtypeStruct((experts, few, width), bf16),
            ),
            in_specs=[any_space] * 3,
            out_specs=(any_space,) * 3,
            scratch_shapes=[
                pltpu.VMEM((experts, few, width), bf16),
                pltpu.VMEM((rows, width), bf16),
                pltpu.VMEM((dp, depth, rank), bf16),
                pltpu.VMEM((dp - 1, experts, few, depth), bf16),
                pltpu.VMEM((dp, rows, rank), f32),
                pltpu.VMEM((rank, 2 * rank), f32),
                pltpu.VMEM((dp, rows, rank), bf16),
                pltpu.VMEM((rank, depth), f32),
                pltpu.VMEM((dp, rank, depth), bf16),
                pltpu.VMEM((layers, rank, depth), bf16),
                pltpu.VMEM((layers, dp, group * few, rank), bf16),
                pltpu.VMEM((layers, dp, group * few, depth), bf16),
                pltpu.VMEM((depth, rank), bf16),
                pltpu.VMEM((dp, SIDE, rank), f32),
                dma((experts,)),
                dma((experts,)),
                dma((dp - 1, experts)),
                dma((dp - 1, experts)),
                dma((dp - 1, experts)),
                dma((dp - 1, experts)),
                dma((dp - 1,)),
                dma((dp - 1,)),
                dma((dp - 1,)),
                dma((dp - 1,)),
                dma((dp - 1,)),
                dma((dp - 1,)),
                dma((layers,)),
                dma((layers,)),
                dma((layers, pieces, 2)),
                dma((layers, pieces)),
                dma((layers, team - 1)),
                dma((layers, team)),
                dma((3,)),
            ],
            compiler_params=pltpu.CompilerParams(
                collective_id=0, has_side_effects=True, vmem_limit_bytes=66000000
            ),
            name="dion_step",
        )(gradients, momentum[0], right_factor[0])
        return kept[None], own_factor[None], returned

    return body


def solution(mesh):
    in_specs = (P(None, ("dp", "expert"), None), P("expert", "dp", None), P("expert", "dp", None))
    out_specs = (P("expert", "dp", None), P("expert", "dp", None), P(None, ("dp", "expert"), None))
    return jax.shard_map(
        make_body(mesh.shape["dp"]),
        mesh=mesh,
        in_specs=in_specs,
        out_specs=out_specs,
        check_vma=False,
    )
```

```python
import functools
import math

import jax
import jax.numpy as jnp
from jax import lax
from jax.experimental import pallas as pl
from jax.experimental.pallas import tpu as pltpu
from jax.sharding import PartitionSpec as P

decay_rate = 0.95
epsilon = 1e-06
PIECES = 4
AHEAD = 1
LANES = 128
SIDE = 32
SUBLANES = 8
MESH = pl.DeviceIdType.MESH


def exact_dot(a, b, contract):
    return lax.dot_general(
        a,
        b,
        (((contract[0],), (contract[1],)), ((), ())),
        precision=lax.Precision.HIGHEST,
        preferred_element_type=jnp.float32,
    )


def dot(a, b, contract=(1, 0)):
    return lax.dot_general(
        a, b, (((contract[0],), (contract[1],)), ((), ())), preferred_element_type=jnp.float32
    )


def factor_inverse(work, rank):
    block = min(LANES, rank)
    sub = lax.broadcasted_iota(jnp.int32, (SIDE, LANES), 0)
    lane = lax.broadcasted_iota(jnp.int32, (SIDE, block), 1)
    for start in range(0, rank, block):
        end = start + block
        low, high = start, rank + end
        tiles = (high - low) // LANES
        place = lax.broadcasted_iota(jnp.int32, (block, high - low), 0)

        def panel(step, _, start=start, end=end, low=low, high=high, tiles=tiles, place=place):
            first = pl.multiple_of(step * SIDE, SIDE)
            rows = work[pl.ds(start + first, SIDE), low:high]
            square = rows[:, :block]
            columns = [
                jnp.broadcast_to(
                    jnp.sum(jnp.where(lane == first + j, square, 0.0), axis=1, keepdims=True),
                    (SIDE, LANES),
                )
                for j in range(SIDE)
            ]
            parts = [rows[:, LANES * t : LANES * (t + 1)] for t in range(tiles)]
            roots = jnp.zeros((SIDE, LANES), jnp.float32)
            for j in range(SIDE):
                root = lax.rsqrt(jnp.broadcast_to(columns[j][j : j + 1, :], (SIDE, LANES)))
                roots = jnp.where(sub == j, root, roots)
                column = jnp.where(sub > j, columns[j] * root, 0.0)
                for k in range(j + 1, SIDE):
                    columns[k] = columns[k] - column * jnp.broadcast_to(
                        column[k : k + 1, :], (SIDE, LANES)
                    )
                column = column * root
                for t in range(tiles):
                    pivot = jnp.broadcast_to(parts[t][j : j + 1, :], (SIDE, LANES))
                    parts[t] = parts[t] - column * pivot
            rows = jnp.concatenate([part * roots for part in parts], axis=1)
            work[pl.ds(start + first, SIDE), low:high] = rows
            change = exact_dot(rows[:, :block], rows, (0, 0))
            old = work[start:end, low:high]
            work[start:end, low:high] = jnp.where(place >= first + SIDE, old - change, old)
            return 0

        lax.fori_loop(0, block // SIDE, panel, 0)
        if end < rank:
            done = work[start:end, low:high]
            work[end:, low:high] = work[end:, low:high] - exact_dot(
                done[:, block : rank - low], done, (0, 0)
            )


def cuts(depth):
    tiles = depth // LANES
    pieces = min(PIECES, tiles)
    edges = [-(-tiles * k // pieces) * LANES for k in range(pieces + 1)]
    return list(zip(edges[:-1], edges[1:]))


def step_kernel(
    dp,
    experts,
    layers,
    gradients,
    momentum,
    right_factor,
    kept_out,
    factor_out,
    update_out,
    blended,
    held,
    factor,
    other,
    left,
    work,
    ortho,
    right,
    rounded,
    pair,
    normal,
    rows_in,
    update,
    turned,
    sums,
    grad_send,
    grad_recv,
    half_send,
    half_recv,
    left_send,
    left_recv,
    pair_send,
    pair_recv,
    sum_send,
    sum_recv,
    round_send,
    round_recv,
    rows_send,
    rows_recv,
    normal_send,
    normal_recv,
    update_send,
    update_recv,
    local_sem,
):
    x = lax.axis_index("dp")
    e = lax.axis_index("expert")
    group = experts // layers
    z, s = e // group, lax.rem(e, group)
    few = gradients.shape[1]
    rows, width = momentum.shape
    depth, rank = right_factor.shape
    team = dp * group
    mine = x * group + s
    pieces = cuts(depth)

    def remote(src, dst, send, recv, to_x, to_e):
        return pltpu.make_async_remote_copy(
            src_ref=src,
            dst_ref=dst,
            send_sem=send,
            recv_sem=recv,
            device_id=(to_x, to_e),
            device_id_type=MESH,
        )

    def mate(k):
        return lax.rem(x + k, dp)

    def away(t):
        apart = (t + 1) // 2
        to = jnp.where(lax.rem(t, 2) == 1, z + apart, z - apart)
        return to, (to >= 0) & (to < layers)

    barrier = pltpu.get_barrier_semaphore()

    def greet_expert(k, _):
        pl.semaphore_signal(
            barrier, inc=1, device_id=(x, lax.rem(e + k, experts)), device_id_type=MESH
        )
        return 0

    lax.fori_loop(1, experts, greet_expert, 0)
    for k in range(1, dp):
        for m in range(group):
            pl.semaphore_signal(
                barrier, inc=1, device_id=(mate(k), z * group + m), device_id_type=MESH
            )
    local_momentum = pltpu.make_async_copy(momentum, held, local_sem.at[0])
    local_momentum.start()
    local_factor = pltpu.make_async_copy(right_factor, factor.at[x], local_sem.at[1])
    local_factor.start()
    local_grad = pltpu.make_async_copy(gradients.at[e], blended.at[e], local_sem.at[2])
    local_grad.start()
    pl.semaphore_wait(barrier, experts - 1 + (dp - 1) * group)

    factor_copies = [
        remote(right_factor, factor.at[x], pair_send.at[k - 1], pair_recv.at[k - 1], mate(k), e)
        for k in range(1, dp)
    ]
    for copy in factor_copies:
        copy.start()

    def grad_copy(to):
        return remote(
            gradients.at[to], blended.at[e], grad_send.at[to], grad_recv.at[e], x, to
        )

    def send_layer(t, _):
        near, real = away(jnp.maximum(t - 2, 0))
        end = (near == 0) | (near == layers - 1)
        to = jnp.where(t < 2, t * (layers - 1), near)
        real = jnp.where(t < 2, to != z, real & ((near == z) | ~end))

        @pl.when(real)
        def _():
            def one(k, _):
                m = lax.rem(s + k, group)

                @pl.when(to * group + m != e)
                def _():
                    grad_copy(to * group + m).start()

                return 0

            lax.fori_loop(0, group, one, 0)

        return 0

    lax.fori_loop(0, 2 * layers + 1, send_layer, 0)
    local_momentum.wait()
    local_factor.wait()
    local_grad.wait()
    for copy in factor_copies:
        copy.wait_recv()

    def half_copy(k, block):
        to = mate(k)
        return remote(
            blended.at[block, :, pl.ds(pl.multiple_of(to * depth, LANES), depth)],
            other.at[k - 1, block],
            half_send.at[k - 1, block],
            half_recv.at[k - 1, block],
            to,
            e,
        )

    def left_copy(k, block):
        part = left.at[x, pl.ds(pl.multiple_of(block * few, few), few)]
        return remote(
            part, part, left_send.at[k - 1, block], left_recv.at[k - 1, block], mate(k), e
        )

    def take_layer(t, _):
        inner, real = away(jnp.clip(2 * layers + 1 - t, 0, 2 * layers - 2))
        real = real & (inner != z) & (inner > 0) & (inner < layers - 1)
        near = jnp.where(2 * z < layers, 0, layers - 1)
        end = jnp.where(t == 1, near, layers - 1 - near)
        source = jnp.where(t == 0, z, jnp.where(t < 3, end, inner))
        real = jnp.where(t == 0, True, jnp.where(t < 3, end != z, real))

        @pl.when(real)
        def _():
            def one(k, _):
                block = source * group + lax.rem(s + group - k, group)

                @pl.when(block != e)
                def _():
                    remote(
                        gradients.at[block], blended.at[block],
                        grad_send.at[block], grad_recv.at[block], x, block,
                    ).wait_recv()

                span = pl.ds(pl.multiple_of(block * few, few), few)
                new = (
                    decay_rate * held[span].astype(jnp.float32)
                    + blended[block].astype(jnp.float32)
                ).astype(jnp.bfloat16)
                blended[block] = new
                left[x, span] = dot(new, factor[...].reshape(dp * depth, rank))
                for k in range(1, dp):
                    half_copy(k, block).start()
                    left_copy(k, block).start()
                return 0

            lax.fori_loop(0, group, one, 0)

        return 0

    lax.fori_loop(0, 2 * layers + 1, take_layer, 0)

    def arrived(block, _):
        for k in range(1, dp):
            half_copy(k, block).wait_recv()
            left_copy(k, block).wait_recv()
        return 0

    lax.fori_loop(0, experts, arrived, 0)

    every = left[...].reshape(dp * rows, rank)
    row = lax.broadcasted_iota(jnp.int32, (rank, rank), 0)
    col = lax.broadcasted_iota(jnp.int32, (rank, rank), 1)
    work[:, :rank] = exact_dot(every, every, (0, 0))
    work[:, rank:] = jnp.where(row == col, 1.0, 0.0)
    factor_inverse(work, rank)
    inverse = work[:, rank:]
    for k in range(dp):
        ortho[k] = exact_dot(left[k], inverse, (1, 1)).astype(jnp.bfloat16)
    per = group * few

    def rows_copy(source, to):
        return remote(
            ortho.at[:, pl.ds(pl.multiple_of(to * per, per), per)],
            rows_in.at[source],
            rows_send.at[to],
            rows_recv.at[source],
            x,
            to * group + s,
        )

    def send_rows(t, _):
        to, real = away(t)

        @pl.when(real)
        def _():
            rows_copy(z, to).start()

        return 0

    own = jnp.transpose(exact_dot(left[x], inverse, (1, 1))).astype(jnp.bfloat16)
    others = [
        jnp.transpose(exact_dot(left[mate(k)], inverse, (1, 1))).astype(jnp.bfloat16)
        for k in range(1, dp)
    ]
    square = jnp.zeros((rank, LANES), jnp.float32)
    for lo, hi in pieces:
        begin = pl.multiple_of(x * depth + lo, LANES)
        part = dot(own, blended[:, :, pl.ds(begin, hi - lo)].reshape(rows, hi - lo))
        for k in range(1, dp):
            part = part + dot(others[k - 1], other[k - 1, :, :, lo:hi].reshape(rows, hi - lo))
        right[:, lo:hi] = part
        rounded[:, lo:hi] = part.astype(jnp.bfloat16)
        for at in range(0, hi - lo, LANES):
            tile = part[:, at : at + LANES]
            square = square + tile * tile
    square = jnp.broadcast_to(
        jnp.sum(jnp.transpose(square), axis=0, keepdims=True), (SUBLANES, rank)
    )
    sums[0] = square
    lax.fori_loop(1, 2 * layers - 1, send_rows, 0)
    sum_copies = [
        remote(sums.at[0], sums.at[k], sum_send.at[k - 1], sum_recv.at[k - 1], mate(k), e)
        for k in range(1, dp)
    ]
    for copy in sum_copies:
        copy.start()
    total = square
    for k in range(1, dp):
        sum_copies[k - 1].wait_recv()
        total = total + sums[k]
    scale = lax.rsqrt(total[0:1, :] / width + epsilon)
    scale = jnp.transpose(jnp.broadcast_to(scale, (LANES, rank)))[:, 0:1]

    def normal_copy(layer, piece, to, way):
        lo, hi = pieces[piece]
        part = normal.at[layer, :, lo:hi]
        return remote(
            part,
            part,
            normal_send.at[layer, piece, way],
            normal_recv.at[layer, piece],
            x,
            to * group + s,
        )

    is_end = (z == 0) | (z == layers - 1)
    beyond = layers - 1 - z

    def inside(layer):
        return (layer >= 0) & (layer < layers)

    def multiply(layer, piece):
        lo, hi = pieces[piece]
        result = gain * dot(rows_in[layer].reshape(dp * per, rank), normal[layer, :, lo:hi])
        update[layer, :, :, lo:hi] = result.astype(jnp.bfloat16).reshape(dp, per, hi - lo)

    def multiply_own(half, piece, source):
        lo, hi = pieces[piece]
        begin = pl.multiple_of(half * depth + lo, LANES)
        result = gain * dot(ortho[x, pl.ds(pl.multiple_of(z * per, per), per)], source[:, lo:hi])
        update[z, half, :, lo:hi] = result.astype(jnp.bfloat16)

        def place(to_s):
            return (
                update.at[z, half, pl.ds(pl.multiple_of(to_s * few, few), few), lo:hi],
                update_out.at[e, :, pl.ds(begin, hi - lo)],
            )

        src, dst = place(s)
        pltpu.make_async_copy(src, dst, update_recv.at[z, mine]).start()

        def one(k, _):
            to_s = lax.rem(s + k, group)
            src, dst = place(to_s)
            remote(
                src, dst, update_send.at[z, k - 1], update_recv.at[z, mine], x, z * group + to_s
            ).start()
            return 0

        lax.fori_loop(1, group, one, 0)

    def scatter(layer, piece):
        lo, hi = pieces[piece]
        begin = pl.multiple_of(x * depth + lo, LANES)

        def place(to_x, to_s):
            return (
                update.at[layer, to_x, pl.ds(pl.multiple_of(to_s * few, few), few), lo:hi],
                update_out.at[layer * group + s, :, pl.ds(begin, hi - lo)],
            )

        src, dst = place(x, s)
        pltpu.make_async_copy(src, dst, update_recv.at[layer, mine]).start()

        def one(k, _):
            to = lax.rem(mine + k, team)
            to_x, to_s = to // group, lax.rem(to, group)
            src, dst = place(to_x, to_s)
            remote(
                src,
                dst,
                update_send.at[layer, k - 1],
                update_recv.at[layer, mine],
                to_x,
                z * group + to_s,
            ).start()
            return 0

        lax.fori_loop(1, team, one, 0)

    gain = math.sqrt(rows * dp / rank)
    for piece, (lo, hi) in enumerate(pieces):
        normal[z, :, lo:hi] = (right[:, lo:hi] * scale).astype(jnp.bfloat16)

    def onward(layer, side):
        to = z + side
        last = ((layer == 0) & (to == layers - 1)) | ((layer == layers - 1) & (to == 0))
        return inside(to) & (side * (z - layer) >= 0) & ~last

    for piece in range(len(pieces)):
        if piece == AHEAD:

            @pl.when(is_end & (z != beyond))
            def _():
                for whole in range(len(pieces)):
                    normal_copy(z, whole, beyond, 2).start()

        for side in (1, -1):

            @pl.when(onward(z, side))
            def _(piece=piece, side=side):
                normal_copy(z, piece, z + side, (side + 1) // 2).start()

    pair_copies = [
        remote(normal.at[z], pair.at[k - 1], round_send.at[k - 1], round_recv.at[k - 1], mate(k), e)
        for k in range(1, dp)
    ]
    for copy in pair_copies:
        copy.start()
    for piece in range(len(pieces)):
        multiply_own(x, piece, normal.at[z])

    turned[...] = jnp.transpose(normal[z].astype(jnp.float32)).astype(jnp.bfloat16)
    factor_store = pltpu.make_async_copy(turned, factor_out, local_sem.at[1])
    factor_store.start()

    def keep(half):
        for lo, hi in pieces:
            at = pl.ds(pl.multiple_of(half * depth + lo, LANES), hi - lo)
            old = blended[:, :, at].reshape(rows, hi - lo).astype(jnp.float32)
            held[:, at] = (
                old - (1.0 - decay_rate) * dot(ortho[x], rounded[:, lo:hi])
            ).astype(jnp.bfloat16)

    keep(x)

    def come(layer, piece, side):
        normal_copy(layer, piece, z, 0).wait_recv()

        @pl.when(onward(layer, side))
        def _():
            normal_copy(layer, piece, z + side, (side + 1) // 2).start()

        multiply(layer, piece)
        scatter(layer, piece)

    @pl.when(is_end & (z != beyond))
    def _():
        rows_copy(beyond, z).wait_recv()
        for piece in range(len(pieces)):
            normal_copy(beyond, piece, z, 0).wait_recv()
            multiply(beyond, piece)
            scatter(beyond, piece)

    def far(apart, _):
        for side in (1, -1):

            @pl.when(inside(z - side * apart))
            def _(side=side):
                rows_copy(z - side * apart, z).wait_recv()

        for piece in range(len(pieces)):
            for side in (1, -1):

                @pl.when(inside(z - side * apart))
                def _(piece=piece, side=side):
                    come(z - side * apart, piece, side)

        @pl.when(apart == 1)
        def _():
            partners()

        return 0

    def partners():
        for k in range(1, dp):
            pair_copies[k - 1].wait_recv()
            for piece, (lo, hi) in enumerate(pieces):
                multiply_own(mate(k), piece, pair.at[k - 1])
                rounded[:, lo:hi] = (
                    pair[k - 1, :, lo:hi].astype(jnp.float32) / scale
                ).astype(jnp.bfloat16)
            keep(mate(k))

    if layers < 3:
        partners()
    lax.fori_loop(1, layers - 1, far, 0)
    kept_store = pltpu.make_async_copy(held, kept_out, local_sem.at[0])
    kept_store.start()

    def done_block(block, _):
        @pl.when(block != e)
        def _():
            grad_copy(block).wait_send()

        for k in range(1, dp):
            half_copy(k, block).wait_send()
            left_copy(k, block).wait_send()
        return 0

    lax.fori_loop(0, experts, done_block, 0)
    for copy in factor_copies + sum_copies + pair_copies:
        copy.wait_send()

    def done_layer(layer, _):
        @pl.when(layer != z)
        def _():
            rows_copy(z, layer).wait_send()

        for piece in range(len(pieces)):
            for side in (1, -1):
                @pl.when(onward(layer, side))
                def _(piece=piece, side=side):
                    normal_copy(layer, piece, z, (side + 1) // 2).wait_send()

            @pl.when((layer == beyond) & (layer != z) & is_end)
            def _(piece=piece):
                normal_copy(z, piece, layer, 2).wait_send()

        @pl.when(layer == z)
        def _():
            def gone(k, _):
                remote(
                    gradients.at[0], update_out.at[e],
                    update_send.at[z, k - 1], update_recv.at[z, mine], mate(1), e,
                ).wait_send()
                return 0

            lax.fori_loop(1, group, gone, 0)

            def came(m, _):
                pltpu.make_async_copy(
                    gradients.at[0], update_out.at[e], update_recv.at[z, x * group + m]
                ).wait()
                return 0

            lax.fori_loop(0, group, came, 0)

        @pl.when(layer != z)
        def _():
            src = update.at[layer, 0, pl.ds(0, few)]
            dst = update_out.at[layer * group, :, pl.ds(0, depth)]

            def gone(k, _):
                remote(
                    src, dst, update_send.at[layer, k - 1], update_recv.at[layer, mine], mate(1), e
                ).wait_send()
                return 0

            lax.fori_loop(1, team, gone, 0)

            def came(m, _):
                pltpu.make_async_copy(src, dst, update_recv.at[layer, m]).wait()
                return 0

            lax.fori_loop(0, team, came, 0)

        return 0

    lax.fori_loop(0, layers, done_layer, 0)
    factor_store.wait()
    kept_store.wait()


def make_body(dp):
    def body(gradients, momentum, right_factor):
        experts, few, width = gradients.shape
        rows = momentum.shape[1]
        depth, rank = right_factor.shape[1:]
        group = max(1, min(experts, rank // (dp * few)))
        while experts % group:
            group -= 1
        layers = experts // group
        team = dp * group
        pieces = len(cuts(depth))
        any_space = pl.BlockSpec(memory_space=pl.ANY)
        bf16, f32 = jnp.bfloat16, jnp.float32
        dma = pltpu.SemaphoreType.DMA
        kept, own_factor, returned = pl.pallas_call(
            functools.partial(step_kernel, dp, experts, layers),
            out_shape=(
                jax.ShapeDtypeStruct((rows, width), bf16),
                jax.ShapeDtypeStruct((depth, rank), bf16),
                jax.ShapeDtypeStruct((experts, few, width), bf16),
            ),
            in_specs=[any_space] * 3,
            out_specs=(any_space,) * 3,
            scratch_shapes=[
                pltpu.VMEM((experts, few, width), bf16),
                pltpu.VMEM((rows, width), bf16),
                pltpu.VMEM((dp, depth, rank), bf16),
                pltpu.VMEM((dp - 1, experts, few, depth), bf16),
                pltpu.VMEM((dp, rows, rank), f32),
                pltpu.VMEM((rank, 2 * rank), f32),
                pltpu.VMEM((dp, rows, rank), bf16),
                pltpu.VMEM((rank, depth), f32),
                pltpu.VMEM((rank, depth), bf16),
                pltpu.VMEM((dp - 1, rank, depth), bf16),
                pltpu.VMEM((layers, rank, depth), bf16),
                pltpu.VMEM((layers, dp, group * few, rank), bf16),
                pltpu.VMEM((layers, dp, group * few, depth), bf16),
                pltpu.VMEM((depth, rank), bf16),
                pltpu.VMEM((dp, SUBLANES, rank), f32),
                dma((experts,)),
                dma((experts,)),
                dma((dp - 1, experts)),
                dma((dp - 1, experts)),
                dma((dp - 1, experts)),
                dma((dp - 1, experts)),
                dma((dp - 1,)),
                dma((dp - 1,)),
                dma((dp - 1,)),
                dma((dp - 1,)),
                dma((dp - 1,)),
                dma((dp - 1,)),
                dma((layers,)),
                dma((layers,)),
                dma((layers, pieces, 3)),
                dma((layers, pieces)),
                dma((layers, team - 1)),
                dma((layers, team)),
                dma((3,)),
            ],
            compiler_params=pltpu.CompilerParams(
                collective_id=0, has_side_effects=True, vmem_limit_bytes=66000000
            ),
            name="dion_step",
        )(gradients, momentum[0], right_factor[0])
        return kept[None], own_factor[None], returned

    return body


def solution(mesh):
    in_specs = (P(None, ("dp", "expert"), None), P("expert", "dp", None), P("expert", "dp", None))
    out_specs = (P("expert", "dp", None), P("expert", "dp", None), P(None, ("dp", "expert"), None))
    return jax.shard_map(
        make_body(mesh.shape["dp"]),
        mesh=mesh,
        in_specs=in_specs,
        out_specs=out_specs,
        check_vma=False,
    )
```

```python
import functools
import math

import jax
import jax.numpy as jnp
from jax import lax
from jax.experimental import pallas as pl
from jax.experimental.pallas import tpu as pltpu
from jax.sharding import PartitionSpec as P

decay_rate = 0.95
epsilon = 1e-06
PIECES = 4
LANES = 128
SIDE = 32
SUBLANES = 8
MESH = pl.DeviceIdType.MESH


def exact_dot(a, b, contract):
    return lax.dot_general(
        a,
        b,
        (((contract[0],), (contract[1],)), ((), ())),
        precision=lax.Precision.HIGHEST,
        preferred_element_type=jnp.float32,
    )


def dot(a, b, contract=(1, 0)):
    return lax.dot_general(
        a, b, (((contract[0],), (contract[1],)), ((), ())), preferred_element_type=jnp.float32
    )


def factor_inverse(work, rank):
    block = min(LANES, rank)
    sub = lax.broadcasted_iota(jnp.int32, (SIDE, LANES), 0)
    lane = lax.broadcasted_iota(jnp.int32, (SIDE, block), 1)
    for start in range(0, rank, block):
        end = start + block
        low, high = start, rank + end
        tiles = (high - low) // LANES
        place = lax.broadcasted_iota(jnp.int32, (block, high - low), 0)

        def panel(step, _, start=start, end=end, low=low, high=high, tiles=tiles, place=place):
            first = pl.multiple_of(step * SIDE, SIDE)
            rows = work[pl.ds(start + first, SIDE), low:high]
            square = rows[:, :block]
            columns = [
                jnp.broadcast_to(
                    jnp.sum(jnp.where(lane == first + j, square, 0.0), axis=1, keepdims=True),
                    (SIDE, LANES),
                )
                for j in range(SIDE)
            ]
            parts = [rows[:, LANES * t : LANES * (t + 1)] for t in range(tiles)]
            roots = jnp.zeros((SIDE, LANES), jnp.float32)
            for j in range(SIDE):
                root = lax.rsqrt(jnp.broadcast_to(columns[j][j : j + 1, :], (SIDE, LANES)))
                roots = jnp.where(sub == j, root, roots)
                column = jnp.where(sub > j, columns[j] * root, 0.0)
                for k in range(j + 1, SIDE):
                    columns[k] = columns[k] - column * jnp.broadcast_to(
                        column[k : k + 1, :], (SIDE, LANES)
                    )
                column = column * root
                for t in range(tiles):
                    pivot = jnp.broadcast_to(parts[t][j : j + 1, :], (SIDE, LANES))
                    parts[t] = parts[t] - column * pivot
            rows = jnp.concatenate([part * roots for part in parts], axis=1)
            work[pl.ds(start + first, SIDE), low:high] = rows
            change = exact_dot(rows[:, :block], rows, (0, 0))
            old = work[start:end, low:high]
            work[start:end, low:high] = jnp.where(place >= first + SIDE, old - change, old)
            return 0

        lax.fori_loop(0, block // SIDE, panel, 0)
        if end < rank:
            done = work[start:end, low:high]
            work[end:, low:high] = work[end:, low:high] - exact_dot(
                done[:, block : rank - low], done, (0, 0)
            )


def cuts(depth):
    tiles = depth // LANES
    pieces = min(PIECES, tiles)
    edges = [-(-tiles * k // pieces) * LANES for k in range(pieces + 1)]
    return list(zip(edges[:-1], edges[1:]))


def step_kernel(
    dp,
    experts,
    layers,
    gradients,
    momentum,
    right_factor,
    held,
    turned,
    update_out,
    blended,
    factor,
    other,
    left,
    work,
    ortho,
    right,
    rounded,
    pair,
    normal,
    rows_in,
    update,
    sums,
    grad_send,
    grad_recv,
    half_send,
    half_recv,
    left_send,
    left_recv,
    pair_send,
    pair_recv,
    sum_send,
    sum_recv,
    round_send,
    round_recv,
    rows_send,
    rows_recv,
    normal_send,
    normal_recv,
    update_send,
    update_recv,
    local_sem,
):
    x = lax.axis_index("dp")
    e = lax.axis_index("expert")
    group = experts // layers
    z, s = e // group, lax.rem(e, group)
    few = gradients.shape[1]
    rows, width = momentum.shape
    depth, rank = right_factor.shape
    team = dp * group
    mine = x * group + s
    pieces = cuts(depth)

    def remote(src, dst, send, recv, to_x, to_e):
        return pltpu.make_async_remote_copy(
            src_ref=src,
            dst_ref=dst,
            send_sem=send,
            recv_sem=recv,
            device_id=(to_x, to_e),
            device_id_type=MESH,
        )

    def mate(k):
        return lax.rem(x + k, dp)

    near_end = jnp.where(2 * z < layers, 0, layers - 1)

    def away(t):
        apart = (t + 1) // 2
        to = jnp.where(lax.rem(t, 2) == 1, z + apart, z - apart)
        return to, (to >= 0) & (to < layers)

    barrier = pltpu.get_barrier_semaphore()

    def greet_expert(k, _):
        pl.semaphore_signal(
            barrier, inc=1, device_id=(x, lax.rem(e + k, experts)), device_id_type=MESH
        )
        return 0

    lax.fori_loop(1, experts, greet_expert, 0)
    for k in range(1, dp):
        for m in range(group):
            pl.semaphore_signal(
                barrier, inc=1, device_id=(mate(k), z * group + m), device_id_type=MESH
            )
    local_momentum = pltpu.make_async_copy(momentum, held, local_sem.at[0])
    local_momentum.start()
    local_factor = pltpu.make_async_copy(right_factor, factor.at[x], local_sem.at[1])
    local_factor.start()
    local_grad = pltpu.make_async_copy(gradients.at[e], blended.at[e], local_sem.at[2])
    local_grad.start()
    pl.semaphore_wait(barrier, experts - 1 + (dp - 1) * group)

    factor_copies = [
        remote(right_factor, factor.at[x], pair_send.at[k - 1], pair_recv.at[k - 1], mate(k), e)
        for k in range(1, dp)
    ]
    for copy in factor_copies:
        copy.start()

    def grad_copy(to):
        return remote(
            gradients.at[to], blended.at[e], grad_send.at[to], grad_recv.at[e], x, to
        )

    def send_layer(t, _):
        last = t > 2 * layers - 2
        inner, real = away(jnp.minimum(t, 2 * layers - 2))
        real = real & ((inner == z) | ((inner > 0) & (inner < layers - 1)))
        end = jnp.where(t == 2 * layers - 1, near_end, layers - 1 - near_end)
        to = jnp.where(last, end, inner)
        real = jnp.where(last, end != z, real)

        @pl.when(real)
        def _():
            def one(k, _):
                m = lax.rem(s + k, group)

                @pl.when(to * group + m != e)
                def _():
                    grad_copy(to * group + m).start()

                return 0

            lax.fori_loop(0, group, one, 0)

        return 0

    lax.fori_loop(0, 2 * layers + 1, send_layer, 0)
    local_momentum.wait()
    local_factor.wait()
    local_grad.wait()
    for copy in factor_copies:
        copy.wait_recv()

    def half_copy(k, block):
        to = mate(k)
        return remote(
            blended.at[block, :, pl.ds(pl.multiple_of(to * depth, LANES), depth)],
            other.at[k - 1, block],
            half_send.at[k - 1, block],
            half_recv.at[k - 1, block],
            to,
            e,
        )

    def left_copy(k, block):
        part = left.at[x, pl.ds(pl.multiple_of(block * few, few), few)]
        return remote(
            part, part, left_send.at[k - 1, block], left_recv.at[k - 1, block], mate(k), e
        )

    def take_layer(t, _):
        at_end = (z == 0) | (z == layers - 1)
        source, real = away(jnp.where(at_end & (t > 2), 2 * layers + 1 - t, t))

        @pl.when(real)
        def _():
            def one(k, _):
                block = source * group + lax.rem(s + group - k, group)

                @pl.when(block != e)
                def _():
                    remote(
                        gradients.at[block], blended.at[block],
                        grad_send.at[block], grad_recv.at[block], x, block,
                    ).wait_recv()

                span = pl.ds(pl.multiple_of(block * few, few), few)
                new = (
                    decay_rate * held[span].astype(jnp.float32)
                    + blended[block].astype(jnp.float32)
                ).astype(jnp.bfloat16)
                blended[block] = new
                left[x, span] = dot(new, factor[...].reshape(dp * depth, rank))
                for k in range(1, dp):
                    left_copy(k, block).start()
                    half_copy(k, block).start()
                return 0

            lax.fori_loop(0, group, one, 0)

        return 0

    lax.fori_loop(0, 2 * layers - 1, take_layer, 0)

    def left_arrived(block, _):
        for k in range(1, dp):
            left_copy(k, block).wait_recv()
        return 0

    lax.fori_loop(0, experts, left_arrived, 0)

    every = left[...].reshape(dp * rows, rank)
    row = lax.broadcasted_iota(jnp.int32, (rank, rank), 0)
    col = lax.broadcasted_iota(jnp.int32, (rank, rank), 1)
    work[:, :rank] = exact_dot(every, every, (0, 0))
    work[:, rank:] = jnp.where(row == col, 1.0, 0.0)
    factor_inverse(work, rank)
    inverse = work[:, rank:]
    for k in range(dp):
        ortho[k] = exact_dot(left[k], inverse, (1, 1)).astype(jnp.bfloat16)
    per = group * few

    def rows_copy(source, to):
        return remote(
            ortho.at[:, pl.ds(pl.multiple_of(to * per, per), per)],
            rows_in.at[source],
            rows_send.at[to],
            rows_recv.at[source],
            x,
            to * group + s,
        )

    def send_rows(t, _):
        to, real = away(t)

        @pl.when(real)
        def _():
            rows_copy(z, to).start()

        return 0

    own = jnp.transpose(exact_dot(left[x], inverse, (1, 1))).astype(jnp.bfloat16)
    others = [
        jnp.transpose(exact_dot(left[mate(k)], inverse, (1, 1))).astype(jnp.bfloat16)
        for k in range(1, dp)
    ]

    def half_arrived(block, _):
        for k in range(1, dp):
            half_copy(k, block).wait_recv()
        return 0

    lax.fori_loop(0, experts, half_arrived, 0)
    square = jnp.zeros((rank, LANES), jnp.float32)
    for lo, hi in pieces:
        begin = pl.multiple_of(x * depth + lo, LANES)
        part = dot(own, blended[:, :, pl.ds(begin, hi - lo)].reshape(rows, hi - lo))
        for k in range(1, dp):
            part = part + dot(others[k - 1], other[k - 1, :, :, lo:hi].reshape(rows, hi - lo))
        right[:, lo:hi] = part
        rounded[:, lo:hi] = part.astype(jnp.bfloat16)
        for at in range(0, hi - lo, LANES):
            tile = part[:, at : at + LANES]
            square = square + tile * tile
    square = jnp.broadcast_to(
        jnp.sum(jnp.transpose(square), axis=0, keepdims=True), (SUBLANES, rank)
    )
    sums[0] = square
    sum_copies = [
        remote(sums.at[0], sums.at[k], sum_send.at[k - 1], sum_recv.at[k - 1], mate(k), e)
        for k in range(1, dp)
    ]
    for copy in sum_copies:
        copy.start()
    lax.fori_loop(1, 2 * layers - 1, send_rows, 0)
    total = square
    for k in range(1, dp):
        sum_copies[k - 1].wait_recv()
        total = total + sums[k]
    scale = lax.rsqrt(total[0:1, :] / width + epsilon)
    scale = jnp.transpose(jnp.broadcast_to(scale, (LANES, rank)))[:, 0:1]

    def normal_copy(layer, piece, to, way):
        lo, hi = pieces[piece]
        part = normal.at[layer, :, lo:hi]
        return remote(
            part,
            part,
            normal_send.at[layer, piece, way],
            normal_recv.at[layer, piece],
            x,
            to * group + s,
        )

    def inside(layer):
        return (layer >= 0) & (layer < layers)

    def multiply(layer, piece):
        lo, hi = pieces[piece]
        result = gain * dot(rows_in[layer].reshape(dp * per, rank), normal[layer, :, lo:hi])
        update[layer, :, :, lo:hi] = result.astype(jnp.bfloat16).reshape(dp, per, hi - lo)

    def multiply_own(half, piece, source):
        lo, hi = pieces[piece]
        begin = pl.multiple_of(half * depth + lo, LANES)
        result = gain * dot(ortho[x, pl.ds(pl.multiple_of(z * per, per), per)], source[:, lo:hi])
        update[z, half, :, lo:hi] = result.astype(jnp.bfloat16)

        def place(to_s):
            return (
                update.at[z, half, pl.ds(pl.multiple_of(to_s * few, few), few), lo:hi],
                update_out.at[e, :, pl.ds(begin, hi - lo)],
            )

        src, dst = place(s)
        pltpu.make_async_copy(src, dst, update_recv.at[z, mine]).start()

        def one(k, _):
            to_s = lax.rem(s + k, group)
            src, dst = place(to_s)
            remote(
                src, dst, update_send.at[z, k - 1], update_recv.at[z, mine], x, z * group + to_s
            ).start()
            return 0

        lax.fori_loop(1, group, one, 0)

    def scatter(layer, piece):
        lo, hi = pieces[piece]
        begin = pl.multiple_of(x * depth + lo, LANES)

        def place(to_x, to_s):
            return (
                update.at[layer, to_x, pl.ds(pl.multiple_of(to_s * few, few), few), lo:hi],
                update_out.at[layer * group + s, :, pl.ds(begin, hi - lo)],
            )

        src, dst = place(x, s)
        pltpu.make_async_copy(src, dst, update_recv.at[layer, mine]).start()

        def one(k, _):
            to = lax.rem(mine + k, team)
            to_x, to_s = to // group, lax.rem(to, group)
            src, dst = place(to_x, to_s)
            remote(
                src,
                dst,
                update_send.at[layer, k - 1],
                update_recv.at[layer, mine],
                to_x,
                z * group + to_s,
            ).start()
            return 0

        lax.fori_loop(1, team, one, 0)

    gain = math.sqrt(rows * dp / rank)
    for piece, (lo, hi) in enumerate(pieces):
        normal[z, :, lo:hi] = (right[:, lo:hi] * scale).astype(jnp.bfloat16)

    def onward(layer, side):
        return inside(z + side) & (side * (z - layer) >= 0)

    for piece in range(len(pieces)):
        for side in (1, -1):

            @pl.when(onward(z, side))
            def _(piece=piece, side=side):
                normal_copy(z, piece, z + side, (side + 1) // 2).start()

    pair_copies = [
        remote(normal.at[z], pair.at[k - 1], round_send.at[k - 1], round_recv.at[k - 1], mate(k), e)
        for k in range(1, dp)
    ]
    for copy in pair_copies:
        copy.start()
    for piece in range(len(pieces)):
        multiply_own(x, piece, normal.at[z])

    turned[...] = jnp.transpose(normal[z].astype(jnp.float32)).astype(jnp.bfloat16)

    def keep(half):
        for lo, hi in pieces:
            at = pl.ds(pl.multiple_of(half * depth + lo, LANES), hi - lo)
            old = blended[:, :, at].reshape(rows, hi - lo).astype(jnp.float32)
            held[:, at] = (
                old - (1.0 - decay_rate) * dot(ortho[x], rounded[:, lo:hi])
            ).astype(jnp.bfloat16)

    keep(x)

    def come(layer, piece):
        normal_copy(layer, piece, z, 0).wait_recv()
        for side in (1, -1):

            @pl.when(onward(layer, side))
            def _(side=side):
                normal_copy(layer, piece, z + side, (side + 1) // 2).start()

        multiply(layer, piece)
        scatter(layer, piece)

    def inner(t, _):
        layer, real = away(t)

        @pl.when(real & (layer > 0) & (layer < layers - 1))
        def _():
            rows_copy(layer, z).wait_recv()
            for piece in range(len(pieces)):
                come(layer, piece)

        return 0

    lax.fori_loop(1, 2 * layers - 1, inner, 0)

    def partners():
        for k in range(1, dp):
            pair_copies[k - 1].wait_recv()
            for piece, (lo, hi) in enumerate(pieces):
                multiply_own(mate(k), piece, pair.at[k - 1])
                rounded[:, lo:hi] = (
                    pair[k - 1, :, lo:hi].astype(jnp.float32) / scale
                ).astype(jnp.bfloat16)
            keep(mate(k))

    partners()
    def end_layer(t, _):
        layer = jnp.where(t == 0, near_end, layers - 1 - near_end)

        @pl.when((layer != z) & ((t == 0) | (layers > 1)))
        def _():
            rows_copy(layer, z).wait_recv()
            for piece in range(len(pieces)):
                come(layer, piece)

        return 0

    lax.fori_loop(0, 2, end_layer, 0)

    def done_block(block, _):
        @pl.when(block != e)
        def _():
            grad_copy(block).wait_send()

        for k in range(1, dp):
            half_copy(k, block).wait_send()
            left_copy(k, block).wait_send()
        return 0

    lax.fori_loop(0, experts, done_block, 0)
    for copy in factor_copies + sum_copies + pair_copies:
        copy.wait_send()

    def done_layer(layer, _):
        @pl.when(layer != z)
        def _():
            rows_copy(z, layer).wait_send()

        for piece in range(len(pieces)):
            for side in (1, -1):
                @pl.when(onward(layer, side))
                def _(piece=piece, side=side):
                    normal_copy(layer, piece, z, (side + 1) // 2).wait_send()

        @pl.when(layer == z)
        def _():
            def gone(k, _):
                remote(
                    gradients.at[0], update_out.at[e],
                    update_send.at[z, k - 1], update_recv.at[z, mine], mate(1), e,
                ).wait_send()
                return 0

            lax.fori_loop(1, group, gone, 0)

            def came(m, _):
                pltpu.make_async_copy(
                    gradients.at[0], update_out.at[e], update_recv.at[z, x * group + m]
                ).wait()
                return 0

            lax.fori_loop(0, group, came, 0)

        @pl.when(layer != z)
        def _():
            src = update.at[layer, 0, pl.ds(0, few)]
            dst = update_out.at[layer * group, :, pl.ds(0, depth)]

            def gone(k, _):
                remote(
                    src, dst, update_send.at[layer, k - 1], update_recv.at[layer, mine], mate(1), e
                ).wait_send()
                return 0

            lax.fori_loop(1, team, gone, 0)

            def came(m, _):
                pltpu.make_async_copy(src, dst, update_recv.at[layer, m]).wait()
                return 0

            lax.fori_loop(0, team, came, 0)

        return 0

    lax.fori_loop(0, layers, done_layer, 0)


def make_body(dp):
    def body(gradients, momentum, right_factor):
        experts, few, width = gradients.shape
        rows = momentum.shape[1]
        depth, rank = right_factor.shape[1:]
        group = max(1, min(experts, rank // (dp * few)))
        while experts % group:
            group -= 1
        layers = experts // group
        team = dp * group
        pieces = len(cuts(depth))
        any_space = pl.BlockSpec(memory_space=pl.ANY)
        bf16, f32 = jnp.bfloat16, jnp.float32
        dma = pltpu.SemaphoreType.DMA
        kept, own_factor, returned = pl.pallas_call(
            functools.partial(step_kernel, dp, experts, layers),
            out_shape=(
                pltpu.VMEM((rows, width), bf16),
                pltpu.VMEM((depth, rank), bf16),
                pltpu.VMEM((experts, few, width), bf16),
            ),
            in_specs=[any_space] * 3,
            out_specs=(pl.BlockSpec(memory_space=pltpu.VMEM),) * 3,
            scratch_shapes=[
                pltpu.VMEM((experts, few, width), bf16),
                pltpu.VMEM((dp, depth, rank), bf16),
                pltpu.VMEM((dp - 1, experts, few, depth), bf16),
                pltpu.VMEM((dp, rows, rank), f32),
                pltpu.VMEM((rank, 2 * rank), f32),
                pltpu.VMEM((dp, rows, rank), bf16),
                pltpu.VMEM((rank, depth), f32),
                pltpu.VMEM((rank, depth), bf16),
                pltpu.VMEM((dp - 1, rank, depth), bf16),
                pltpu.VMEM((layers, rank, depth), bf16),
                pltpu.VMEM((layers, dp, group * few, rank), bf16),
                pltpu.VMEM((layers, dp, group * few, depth), bf16),
                pltpu.VMEM((dp, SUBLANES, rank), f32),
                dma((experts,)),
                dma((experts,)),
                dma((dp - 1, experts)),
                dma((dp - 1, experts)),
                dma((dp - 1, experts)),
                dma((dp - 1, experts)),
                dma((dp - 1,)),
                dma((dp - 1,)),
                dma((dp - 1,)),
                dma((dp - 1,)),
                dma((dp - 1,)),
                dma((dp - 1,)),
                dma((layers,)),
                dma((layers,)),
                dma((layers, pieces, 2)),
                dma((layers, pieces)),
                dma((layers, team - 1)),
                dma((layers, team)),
                dma((3,)),
            ],
            compiler_params=pltpu.CompilerParams(
                collective_id=0, has_side_effects=True, vmem_limit_bytes=46000000
            ),
            name="dion_step",
        )(gradients, momentum[0], right_factor[0])
        return kept[None], own_factor[None], returned

    return body


def solution(mesh):
    in_specs = (P(None, ("dp", "expert"), None), P("expert", "dp", None), P("expert", "dp", None))
    out_specs = (P("expert", "dp", None), P("expert", "dp", None), P(None, ("dp", "expert"), None))
    return jax.shard_map(
        make_body(mesh.shape["dp"]),
        mesh=mesh,
        in_specs=in_specs,
        out_specs=out_specs,
        check_vma=False,
    )
```

```python
import functools
import math

import jax
import jax.numpy as jnp
from jax import lax
from jax.experimental import pallas as pl
from jax.experimental.pallas import tpu as pltpu
from jax.sharding import PartitionSpec as P

decay_rate = 0.95
epsilon = 1e-06
PIECES = 4
LANES = 128
SIDE = 32
SUBLANES = 8
MESH = pl.DeviceIdType.MESH


def exact_dot(a, b, contract):
    return lax.dot_general(
        a,
        b,
        (((contract[0],), (contract[1],)), ((), ())),
        precision=lax.Precision.HIGHEST,
        preferred_element_type=jnp.float32,
    )


def dot(a, b, contract=(1, 0)):
    return lax.dot_general(
        a, b, (((contract[0],), (contract[1],)), ((), ())), preferred_element_type=jnp.float32
    )


def factor_inverse(work, rank):
    block = min(LANES, rank)
    sub = lax.broadcasted_iota(jnp.int32, (SIDE, LANES), 0)
    lane = lax.broadcasted_iota(jnp.int32, (SIDE, block), 1)
    for start in range(0, rank, block):
        end = start + block
        low, high = start, rank + end
        tiles = (high - low) // LANES
        place = lax.broadcasted_iota(jnp.int32, (block, high - low), 0)

        def panel(step, _, start=start, end=end, low=low, high=high, tiles=tiles, place=place):
            first = pl.multiple_of(step * SIDE, SIDE)
            rows = work[pl.ds(start + first, SIDE), low:high]
            square = rows[:, :block]
            columns = [
                jnp.broadcast_to(
                    jnp.sum(jnp.where(lane == first + j, square, 0.0), axis=1, keepdims=True),
                    (SIDE, LANES),
                )
                for j in range(SIDE)
            ]
            parts = [rows[:, LANES * t : LANES * (t + 1)] for t in range(tiles)]
            roots = jnp.zeros((SIDE, LANES), jnp.float32)
            for j in range(SIDE):
                root = lax.rsqrt(jnp.broadcast_to(columns[j][j : j + 1, :], (SIDE, LANES)))
                roots = jnp.where(sub == j, root, roots)
                column = jnp.where(sub > j, columns[j] * root, 0.0)
                for k in range(j + 1, SIDE):
                    columns[k] = columns[k] - column * jnp.broadcast_to(
                        column[k : k + 1, :], (SIDE, LANES)
                    )
                column = column * root
                for t in range(tiles):
                    pivot = jnp.broadcast_to(parts[t][j : j + 1, :], (SIDE, LANES))
                    parts[t] = parts[t] - column * pivot
            rows = jnp.concatenate([part * roots for part in parts], axis=1)
            work[pl.ds(start + first, SIDE), low:high] = rows
            change = exact_dot(rows[:, :block], rows, (0, 0))
            old = work[start:end, low:high]
            work[start:end, low:high] = jnp.where(place >= first + SIDE, old - change, old)
            return 0

        lax.fori_loop(0, block // SIDE, panel, 0)
        if end < rank:
            done = work[start:end, low:high]
            work[end:, low:high] = work[end:, low:high] - exact_dot(
                done[:, block : rank - low], done, (0, 0)
            )


def cuts(depth):
    tiles = depth // LANES
    pieces = min(PIECES, tiles)
    edges = [-(-tiles * k // pieces) * LANES for k in range(pieces + 1)]
    return list(zip(edges[:-1], edges[1:]))


def step_kernel(
    dp,
    experts,
    layers,
    gradients,
    momentum,
    right_factor,
    held,
    turned,
    update_out,
    blended,
    factor,
    other,
    left,
    work,
    ortho,
    right,
    rounded,
    pair,
    normal,
    rows_in,
    update,
    sums,
    grad_send,
    grad_recv,
    half_send,
    half_recv,
    left_send,
    left_recv,
    pair_send,
    pair_recv,
    sum_send,
    sum_recv,
    round_send,
    round_recv,
    rows_send,
    rows_recv,
    share_send,
    share_recv,
    normal_send,
    normal_recv,
    update_send,
    update_recv,
    local_sem,
):
    x = lax.axis_index("dp")
    e = lax.axis_index("expert")
    group = experts // layers
    z, s = e // group, lax.rem(e, group)
    few = gradients.shape[1]
    rows, width = momentum.shape
    depth, rank = right_factor.shape
    team = dp * group
    mine = x * group + s
    pieces = cuts(depth)

    def remote(src, dst, send, recv, to_x, to_e):
        return pltpu.make_async_remote_copy(
            src_ref=src,
            dst_ref=dst,
            send_sem=send,
            recv_sem=recv,
            device_id=(to_x, to_e),
            device_id_type=MESH,
        )

    def mate(k):
        return lax.rem(x + k, dp)

    near_end = jnp.where(2 * z < layers, 0, layers - 1)

    def away(t):
        apart = (t + 1) // 2
        to = jnp.where(lax.rem(t, 2) == 1, z + apart, z - apart)
        return to, (to >= 0) & (to < layers)

    barrier = pltpu.get_barrier_semaphore()

    def greet_expert(k, _):
        pl.semaphore_signal(
            barrier, inc=1, device_id=(x, lax.rem(e + k, experts)), device_id_type=MESH
        )
        return 0

    lax.fori_loop(1, experts, greet_expert, 0)
    for k in range(1, dp):
        for m in range(group):
            pl.semaphore_signal(
                barrier, inc=1, device_id=(mate(k), z * group + m), device_id_type=MESH
            )
    local_momentum = pltpu.make_async_copy(momentum, held, local_sem.at[0])
    local_momentum.start()
    local_factor = pltpu.make_async_copy(right_factor, factor.at[x], local_sem.at[1])
    local_factor.start()
    local_grad = pltpu.make_async_copy(gradients.at[e], blended.at[e], local_sem.at[2])
    local_grad.start()
    pl.semaphore_wait(barrier, experts - 1 + (dp - 1) * group)

    factor_copies = [
        remote(right_factor, factor.at[x], pair_send.at[k - 1], pair_recv.at[k - 1], mate(k), e)
        for k in range(1, dp)
    ]
    for copy in factor_copies:
        copy.start()

    def grad_copy(to):
        return remote(
            gradients.at[to], blended.at[e], grad_send.at[to], grad_recv.at[e], x, to
        )

    def send_layer(t, _):
        last = t > 2 * layers - 2
        inner, real = away(jnp.minimum(t, 2 * layers - 2))
        real = real & ((inner == z) | ((inner > 0) & (inner < layers - 1)))
        end = jnp.where(t == 2 * layers - 1, near_end, layers - 1 - near_end)
        to = jnp.where(last, end, inner)
        real = jnp.where(last, end != z, real)

        @pl.when(real)
        def _():
            def one(k, _):
                m = lax.rem(s + k, group)

                @pl.when(to * group + m != e)
                def _():
                    grad_copy(to * group + m).start()

                return 0

            lax.fori_loop(0, group, one, 0)

        return 0

    lax.fori_loop(0, 2 * layers + 1, send_layer, 0)
    local_momentum.wait()
    local_factor.wait()
    local_grad.wait()
    for copy in factor_copies:
        copy.wait_recv()

    def half_copy(k, block):
        to = mate(k)
        return remote(
            blended.at[block, :, pl.ds(pl.multiple_of(to * depth, LANES), depth)],
            other.at[k - 1, block],
            half_send.at[k - 1, block],
            half_recv.at[k - 1, block],
            to,
            e,
        )

    def left_copy(k, block):
        part = left.at[x, pl.ds(pl.multiple_of(block * few, few), few)]
        return remote(
            part, part, left_send.at[k - 1, block], left_recv.at[k - 1, block], mate(k), e
        )

    def take_layer(t, _):
        at_end = (z == 0) | (z == layers - 1)
        source, real = away(jnp.where(at_end & (t > 2), 2 * layers + 1 - t, t))

        @pl.when(real)
        def _():
            def one(k, _):
                block = source * group + lax.rem(s + group - k, group)

                @pl.when(block != e)
                def _():
                    remote(
                        gradients.at[block], blended.at[block],
                        grad_send.at[block], grad_recv.at[block], x, block,
                    ).wait_recv()

                span = pl.ds(pl.multiple_of(block * few, few), few)
                new = (
                    decay_rate * held[span].astype(jnp.float32)
                    + blended[block].astype(jnp.float32)
                ).astype(jnp.bfloat16)
                blended[block] = new
                left[x, span] = dot(new, factor[...].reshape(dp * depth, rank))
                for k in range(1, dp):
                    left_copy(k, block).start()
                    half_copy(k, block).start()
                return 0

            lax.fori_loop(0, group, one, 0)

        return 0

    lax.fori_loop(0, 2 * layers - 1, take_layer, 0)

    def left_arrived(block, _):
        for k in range(1, dp):
            left_copy(k, block).wait_recv()
        return 0

    lax.fori_loop(0, experts, left_arrived, 0)

    every = left[...].reshape(dp * rows, rank)
    row = lax.broadcasted_iota(jnp.int32, (rank, rank), 0)
    col = lax.broadcasted_iota(jnp.int32, (rank, rank), 1)
    work[:, :rank] = exact_dot(every, every, (0, 0))
    work[:, rank:] = jnp.where(row == col, 1.0, 0.0)
    factor_inverse(work, rank)
    inverse = work[:, rank:]
    for k in range(dp):
        ortho[k] = exact_dot(left[k], inverse, (1, 1)).astype(jnp.bfloat16)
    per = group * few

    def rows_copy(source, to):
        return remote(
            ortho.at[x, pl.ds(pl.multiple_of(to * per, per), per)],
            rows_in.at[source, x],
            rows_send.at[to],
            rows_recv.at[source],
            x,
            to * group + s,
        )

    def share_copy(source, k):
        part = rows_in.at[source, x]
        return remote(
            part, part, share_send.at[k - 1, source], share_recv.at[k - 1, source], mate(k), e
        )

    def send_rows(t, _):
        to, real = away(t)

        @pl.when(real)
        def _():
            rows_copy(z, to).start()

        return 0

    own = jnp.transpose(exact_dot(left[x], inverse, (1, 1))).astype(jnp.bfloat16)
    others = [
        jnp.transpose(exact_dot(left[mate(k)], inverse, (1, 1))).astype(jnp.bfloat16)
        for k in range(1, dp)
    ]

    def half_arrived(block, _):
        for k in range(1, dp):
            half_copy(k, block).wait_recv()
        return 0

    lax.fori_loop(0, experts, half_arrived, 0)
    square = jnp.zeros((rank, LANES), jnp.float32)
    for lo, hi in pieces:
        begin = pl.multiple_of(x * depth + lo, LANES)
        part = dot(own, blended[:, :, pl.ds(begin, hi - lo)].reshape(rows, hi - lo))
        for k in range(1, dp):
            part = part + dot(others[k - 1], other[k - 1, :, :, lo:hi].reshape(rows, hi - lo))
        right[:, lo:hi] = part
        rounded[:, lo:hi] = part.astype(jnp.bfloat16)
        for at in range(0, hi - lo, LANES):
            tile = part[:, at : at + LANES]
            square = square + tile * tile
    square = jnp.broadcast_to(
        jnp.sum(jnp.transpose(square), axis=0, keepdims=True), (SUBLANES, rank)
    )
    sums[0] = square
    sum_copies = [
        remote(sums.at[0], sums.at[k], sum_send.at[k - 1], sum_recv.at[k - 1], mate(k), e)
        for k in range(1, dp)
    ]
    for copy in sum_copies:
        copy.start()
    lax.fori_loop(1, 2 * layers - 1, send_rows, 0)
    total = square
    for k in range(1, dp):
        sum_copies[k - 1].wait_recv()
        total = total + sums[k]
    scale = lax.rsqrt(total[0:1, :] / width + epsilon)
    scale = jnp.transpose(jnp.broadcast_to(scale, (LANES, rank)))[:, 0:1]

    def normal_copy(layer, piece, to, way):
        lo, hi = pieces[piece]
        part = normal.at[layer, :, lo:hi]
        return remote(
            part,
            part,
            normal_send.at[layer, piece, way],
            normal_recv.at[layer, piece],
            x,
            to * group + s,
        )

    def inside(layer):
        return (layer >= 0) & (layer < layers)

    def multiply(layer, piece):
        lo, hi = pieces[piece]
        result = gain * dot(rows_in[layer].reshape(dp * per, rank), normal[layer, :, lo:hi])
        update[layer, :, :, lo:hi] = result.astype(jnp.bfloat16).reshape(dp, per, hi - lo)

    def multiply_own(half, piece, source):
        lo, hi = pieces[piece]
        begin = pl.multiple_of(half * depth + lo, LANES)
        result = gain * dot(ortho[x, pl.ds(pl.multiple_of(z * per, per), per)], source[:, lo:hi])
        update[z, half, :, lo:hi] = result.astype(jnp.bfloat16)

        def place(to_s):
            return (
                update.at[z, half, pl.ds(pl.multiple_of(to_s * few, few), few), lo:hi],
                update_out.at[e, :, pl.ds(begin, hi - lo)],
            )

        src, dst = place(s)
        pltpu.make_async_copy(src, dst, update_recv.at[z, mine]).start()

        def one(k, _):
            to_s = lax.rem(s + k, group)
            src, dst = place(to_s)
            remote(
                src, dst, update_send.at[z, k - 1], update_recv.at[z, mine], x, z * group + to_s
            ).start()
            return 0

        lax.fori_loop(1, group, one, 0)

    def scatter(layer, piece):
        lo, hi = pieces[piece]
        begin = pl.multiple_of(x * depth + lo, LANES)

        def place(to_x, to_s):
            return (
                update.at[layer, to_x, pl.ds(pl.multiple_of(to_s * few, few), few), lo:hi],
                update_out.at[layer * group + s, :, pl.ds(begin, hi - lo)],
            )

        src, dst = place(x, s)
        pltpu.make_async_copy(src, dst, update_recv.at[layer, mine]).start()

        def one(k, _):
            to = lax.rem(mine + k, team)
            to_x, to_s = to // group, lax.rem(to, group)
            src, dst = place(to_x, to_s)
            remote(
                src,
                dst,
                update_send.at[layer, k - 1],
                update_recv.at[layer, mine],
                to_x,
                z * group + to_s,
            ).start()
            return 0

        lax.fori_loop(1, team, one, 0)

    gain = math.sqrt(rows * dp / rank)
    for piece, (lo, hi) in enumerate(pieces):
        normal[z, :, lo:hi] = (right[:, lo:hi] * scale).astype(jnp.bfloat16)

    def onward(layer, side):
        return inside(z + side) & (side * (z - layer) >= 0)

    for piece in range(len(pieces)):
        for side in (1, -1):

            @pl.when(onward(z, side))
            def _(piece=piece, side=side):
                normal_copy(z, piece, z + side, (side + 1) // 2).start()

    def share(layer, wanted):
        @pl.when(wanted & (layer != z))
        def _():
            rows_copy(layer, z).wait_recv()
            for k in range(1, dp):
                share_copy(layer, k).start()

        return 0

    lax.fori_loop(1, layers - 1, lambda layer, _: share(layer, z >= 0), 0)
    pair_copies = [
        remote(normal.at[z], pair.at[k - 1], round_send.at[k - 1], round_recv.at[k - 1], mate(k), e)
        for k in range(1, dp)
    ]
    for copy in pair_copies:
        copy.start()
    for piece in range(len(pieces)):
        multiply_own(x, piece, normal.at[z])

    turned[...] = jnp.transpose(normal[z].astype(jnp.float32)).astype(jnp.bfloat16)

    def keep(half):
        for lo, hi in pieces:
            at = pl.ds(pl.multiple_of(half * depth + lo, LANES), hi - lo)
            old = blended[:, :, at].reshape(rows, hi - lo).astype(jnp.float32)
            held[:, at] = (
                old - (1.0 - decay_rate) * dot(ortho[x], rounded[:, lo:hi])
            ).astype(jnp.bfloat16)

    keep(x)

    def come(layer, piece):
        normal_copy(layer, piece, z, 0).wait_recv()
        for side in (1, -1):

            @pl.when(onward(layer, side))
            def _(side=side):
                normal_copy(layer, piece, z + side, (side + 1) // 2).start()

        if piece == 0:
            for k in range(1, dp):
                share_copy(layer, k).wait_recv()
        multiply(layer, piece)
        scatter(layer, piece)

    def inner(t, _):
        layer, real = away(t)

        @pl.when(real & (layer > 0) & (layer < layers - 1))
        def _():
            for piece in range(len(pieces)):
                come(layer, piece)

        for end in sorted({0, layers - 1}):
            share(end, t == 2)
        return 0

    lax.fori_loop(1, 2 * layers - 1, inner, 0)

    def partners():
        for k in range(1, dp):
            pair_copies[k - 1].wait_recv()
            for piece, (lo, hi) in enumerate(pieces):
                multiply_own(mate(k), piece, pair.at[k - 1])
                rounded[:, lo:hi] = (
                    pair[k - 1, :, lo:hi].astype(jnp.float32) / scale
                ).astype(jnp.bfloat16)
            keep(mate(k))

    partners()
    def end_layer(t, _):
        layer = jnp.where(t == 0, near_end, layers - 1 - near_end)

        @pl.when((layer != z) & ((t == 0) | (layers > 1)))
        def _():
            for piece in range(len(pieces)):
                come(layer, piece)

        return 0

    lax.fori_loop(0, 2, end_layer, 0)

    def done_block(block, _):
        @pl.when(block != e)
        def _():
            grad_copy(block).wait_send()

        for k in range(1, dp):
            half_copy(k, block).wait_send()
            left_copy(k, block).wait_send()
        return 0

    lax.fori_loop(0, experts, done_block, 0)
    for copy in factor_copies + sum_copies + pair_copies:
        copy.wait_send()

    def done_layer(layer, _):
        @pl.when(layer != z)
        def _():
            rows_copy(z, layer).wait_send()
            for k in range(1, dp):
                share_copy(layer, k).wait_send()

        for piece in range(len(pieces)):
            for side in (1, -1):
                @pl.when(onward(layer, side))
                def _(piece=piece, side=side):
                    normal_copy(layer, piece, z, (side + 1) // 2).wait_send()

        @pl.when(layer == z)
        def _():
            def gone(k, _):
                remote(
                    gradients.at[0], update_out.at[e],
                    update_send.at[z, k - 1], update_recv.at[z, mine], mate(1), e,
                ).wait_send()
                return 0

            lax.fori_loop(1, group, gone, 0)

            def came(m, _):
                pltpu.make_async_copy(
                    gradients.at[0], update_out.at[e], update_recv.at[z, x * group + m]
                ).wait()
                return 0

            lax.fori_loop(0, group, came, 0)

        @pl.when(layer != z)
        def _():
            src = update.at[layer, 0, pl.ds(0, few)]
            dst = update_out.at[layer * group, :, pl.ds(0, depth)]

            def gone(k, _):
                remote(
                    src, dst, update_send.at[layer, k - 1], update_recv.at[layer, mine], mate(1), e
                ).wait_send()
                return 0

            lax.fori_loop(1, team, gone, 0)

            def came(m, _):
                pltpu.make_async_copy(src, dst, update_recv.at[layer, m]).wait()
                return 0

            lax.fori_loop(0, team, came, 0)

        return 0

    lax.fori_loop(0, layers, done_layer, 0)


def make_body(dp):
    def body(gradients, momentum, right_factor):
        experts, few, width = gradients.shape
        rows = momentum.shape[1]
        depth, rank = right_factor.shape[1:]
        group = max(1, min(experts, rank // (dp * few)))
        while experts % group:
            group -= 1
        layers = experts // group
        team = dp * group
        pieces = len(cuts(depth))
        any_space = pl.BlockSpec(memory_space=pl.ANY)
        bf16, f32 = jnp.bfloat16, jnp.float32
        dma = pltpu.SemaphoreType.DMA
        kept, own_factor, returned = pl.pallas_call(
            functools.partial(step_kernel, dp, experts, layers),
            out_shape=(
                pltpu.VMEM((rows, width), bf16),
                pltpu.VMEM((depth, rank), bf16),
                pltpu.VMEM((experts, few, width), bf16),
            ),
            in_specs=[any_space] * 3,
            out_specs=(pl.BlockSpec(memory_space=pltpu.VMEM),) * 3,
            scratch_shapes=[
                pltpu.VMEM((experts, few, width), bf16),
                pltpu.VMEM((dp, depth, rank), bf16),
                pltpu.VMEM((dp - 1, experts, few, depth), bf16),
                pltpu.VMEM((dp, rows, rank), f32),
                pltpu.VMEM((rank, 2 * rank), f32),
                pltpu.VMEM((dp, rows, rank), bf16),
                pltpu.VMEM((rank, depth), f32),
                pltpu.VMEM((rank, depth), bf16),
                pltpu.VMEM((dp - 1, rank, depth), bf16),
                pltpu.VMEM((layers, rank, depth), bf16),
                pltpu.VMEM((layers, dp, group * few, rank), bf16),
                pltpu.VMEM((layers, dp, group * few, depth), bf16),
                pltpu.VMEM((dp, SUBLANES, rank), f32),
                dma((experts,)),
                dma((experts,)),
                dma((dp - 1, experts)),
                dma((dp - 1, experts)),
                dma((dp - 1, experts)),
                dma((dp - 1, experts)),
                dma((dp - 1,)),
                dma((dp - 1,)),
                dma((dp - 1,)),
                dma((dp - 1,)),
                dma((dp - 1,)),
                dma((dp - 1,)),
                dma((layers,)),
                dma((layers,)),
                dma((dp - 1, layers)),
                dma((dp - 1, layers)),
                dma((layers, pieces, 2)),
                dma((layers, pieces)),
                dma((layers, team - 1)),
                dma((layers, team)),
                dma((3,)),
            ],
            compiler_params=pltpu.CompilerParams(
                collective_id=0, has_side_effects=True, vmem_limit_bytes=46000000
            ),
            name="dion_step",
        )(gradients, momentum[0], right_factor[0])
        return kept[None], own_factor[None], returned

    return body


def solution(mesh):
    in_specs = (P(None, ("dp", "expert"), None), P("expert", "dp", None), P("expert", "dp", None))
    out_specs = (P("expert", "dp", None), P("expert", "dp", None), P(None, ("dp", "expert"), None))
    return jax.shard_map(
        make_body(mesh.shape["dp"]),
        mesh=mesh,
        in_specs=in_specs,
        out_specs=out_specs,
        check_vma=False,
    )
```
